32 devices in a mesh: group: 4 (over z), shard: 4 (over y, x), side: 2 (over core).
Axes of the slice: x: 2, y: 2, z: 4, core: 2. Of those that a mesh axis runs over, the one named last changes fastest.
Arguments:
- master: float32 [16, 2048, 768], P('group', ('shard', 'side')), may hold values from -0.125 to 0.125
- momentum: float32 [16, 2048, 768], P('group', ('shard', 'side')), may hold values from -24 to 24
- gradient: bfloat16 [16, 2048, 768], P('group', ('shard', 'side')), may hold values from -6 to 6
- up_weight: bfloat16 [16, 768, 2048], P(('group', 'shard'), 'side'), may hold values from -0.125 to 0.125
- down_weight: bfloat16 [16, 768, 2048], P(('group', 'shard'), 'side'), may hold values from -0.21875 to 0.21875
- tokens: bfloat16 [128, 2048], replicated, may hold values from -6 to 6
- routes: int32 [128, 8], replicated, may hold values from 0 to 15, all different within a row; in each aligned block of 128 rows (0 to 127, 128 to 255, ...) at most 128 rows name the same one
- route_weight: float32 [128, 8], replicated, may hold values from 0.1 to 1
Outputs:
- new_master: float32 [16, 2048, 768], P('group', ('shard', 'side'))
- new_momentum: float32 [16, 2048, 768], P('group', ('shard', 'side'))
- combined: bfloat16 [128, 2048], P(('group', 'shard', 'side'))
The draws below stay inside these ranges and needn't reach their ends.
Inputs may be any that keep to these rules, and one draw needn't show every extreme that they name: `routes`: each row names 8 different experts; no expert is named by more than 128 rows, a bound that some block reaches; every expert is named by some row.
All inputs are finite; a program needn't handle non-finite values.
Results may differ from the reference program's by a relative error of at most 0.02.
Values may be sent and summed in bfloat16 or wider, within the bound.
No kernel may reach another device: no remote copies, remote signals or barrier semaphores. Data moves between devices by JAX's collectives and lax.ppermute only.
A program may use at most 128 MiB of HBM per device.

```python
import math
import jax
import jax.numpy as jnp
import numpy as np
from jax import lax

D = 2048
F = 768
TOP = 8
NS_ITERS = 5
CAP = 128
EXPERTS = 16
TOKENS = 128


def block_scale(key, dims, pieces, low, high):
    def one(axis_at, parts):
        heights = jax.random.uniform(jax.random.fold_in(jax.random.fold_in(key, 6), axis_at), (parts,), jnp.float32, low / len(pieces), high / len(pieces))
        return jnp.repeat(jnp.exp(heights), dims[axis_at] // parts).reshape((-1,) + (1,) * (len(dims) - axis_at - 1))

    factor_of = one(*pieces[0])
    for cut in pieces[1:]:
        factor_of = factor_of * one(*cut)
    return factor_of


def shared_out(rng, own, number, rows, count, top, most, slope):
    ranking = jax.random.permutation(rng, count)
    crowded, usual = portions_of(count, rows * top, most, slope, True), portions_of(count, rows * top, most, slope, False)
    places = jnp.arange(count)

    def named(tallies, turn):
        used = int((tallies > 0).sum())
        fixed = max(1, used // 4)
        passed = fixed + (places - fixed + turn * (used - fixed)) % max(1, count - fixed)
        return jnp.zeros((count,), jnp.int32).at[ranking[jnp.where(places < fixed, places, passed)]].set(jnp.asarray(tallies, jnp.int32))

    tallies = jnp.where(number % 4 == 0, named(crowded, number // 4), named(usual, number - number // 4 - 1))
    mixed = jax.random.permutation(jax.random.fold_in(own, 3), count)
    source_of, taker = mixed[0:count // 2 * 2:2], mixed[1:count // 2 * 2:2]
    room = jnp.minimum(tallies[source_of] - 1, most - tallies[taker]) // 2
    room = jnp.where((source_of == ranking[0]) | (taker == ranking[0]) | (tallies[taker] == 0), 0, jnp.maximum(room, 0))
    passed = jax.random.randint(jax.random.fold_in(own, 4), (count // 2,), 0, 1 << 20) % (room + 1)
    tallies = tallies.at[source_of].add(-passed).at[taker].add(passed)
    labels = jnp.searchsorted(jnp.cumsum(tallies), jnp.arange(rows * top), side="right").astype(jnp.int32)
    table = labels.reshape(top, rows).T
    table = table[jax.random.permutation(jax.random.fold_in(own, 1), rows)]
    turn = jax.random.randint(jax.random.fold_in(own, 2), (rows, 1), 0, top)
    return jnp.take_along_axis(table, (jnp.arange(top)[None, :] + turn) % top, axis=1)


def portions_of(count, total, reach, skew, full):
    portions = [(1 << 20) // math.isqrt(standing ** skew) + 1 for standing in range(1, count + 1)]
    largest = reach if full else min(reach, max(-(-total // count), total * portions[0] // sum(portions)))
    least = 1 if total - largest >= count - 1 else 0
    holding, rest = [largest] + [least] * (count - 1), total - largest - least * (count - 1)
    while rest > 0:
        free = [i for i in range(1, count) if holding[i] < largest] or [i for i in range(1, count) if holding[i] < reach]
        whole, budget = sum([portions[i] for i in free]), rest
        for i in free:
            extra = min(reach - holding[i], max(1, budget * portions[i] // whole), rest)
            holding[i] = holding[i] + extra
            rest = rest - extra
    return np.array(holding)


def normal_values(rng, extent, spread, most, pieces=(), kind=jnp.bfloat16):
    factor_of = block_scale(rng, extent, pieces, -0.22, 0.18) if pieces else 1.0
    values = jax.random.normal(rng, extent, jnp.float32) * spread * factor_of
    return jnp.minimum(jnp.maximum(values, -most), most).astype(kind)


def setup_inputs(seed: int = 0) -> dict:
    splits = jax.random.split(jax.random.key(seed), 9)
    master = normal_values(splits[0], (EXPERTS, D, F), D ** -0.5, 0.125, ((0, 4), (1, 8)), jnp.float32)
    momentum = normal_values(splits[1], (EXPERTS, D, F), 4.0, 24.0, ((0, 4), (1, 8)), jnp.float32)
    gradient = normal_values(splits[2], (EXPERTS, D, F), 1.0, 6.0, ((0, 4), (1, 8)))
    up_weight = normal_values(splits[3], (EXPERTS, F, D), D ** -0.5, 0.125, ((0, 16), (1, 2)))
    down_weight = normal_values(splits[4], (EXPERTS, F, D), F ** -0.5, 0.21875, ((0, 16), (1, 2)))
    tokens = normal_values(splits[5], (TOKENS, D), 1.0, 6.0)
    routes_keys = jax.random.split(jax.random.fold_in(splits[6], 1), TOKENS // TOKENS)
    routes_turns = jax.random.permutation(jax.random.fold_in(splits[6], 3), TOKENS // TOKENS)
    routes = jax.vmap(lambda own, number: shared_out(jax.random.fold_in(splits[6], 2), own, number, TOKENS, EXPERTS, TOP, CAP, 2))(routes_keys, routes_turns).reshape((TOKENS, TOP))
    route_weight = jnp.clip(jax.random.uniform(splits[7], (TOKENS, TOP), jnp.float32, 0.1, 1.0), 0.1, 1.0)
    return dict(master=master, momentum=momentum, gradient=gradient, up_weight=up_weight, down_weight=down_weight, tokens=tokens, routes=routes, route_weight=route_weight)


MOMENTUM_BETA = 0.95
LEARN_RATE = 0.08
WEIGHT_DECAY = 0.1
NEWTON_A = 3.4445
NEWTON_B = -4.775
NEWTON_C = 2.0315
EPSILON = 1e-07

def orthogonal(blended):
    values = blended.astype(jnp.float32)
    scale_sum = jnp.sqrt(jnp.sum(values * values))
    current = (values / (scale_sum + EPSILON)).astype(jnp.bfloat16)
    for iteration in range(NS_ITERS):
        wide = current.astype(jnp.float32)
        gram_matrix = jnp.dot(wide.T, wide, preferred_element_type=jnp.float32).astype(jnp.bfloat16)
        gram_wide = gram_matrix.astype(jnp.float32)
        square = jnp.dot(gram_wide, gram_wide, preferred_element_type=jnp.float32)
        mixing = (NEWTON_B * gram_wide + NEWTON_C * square).astype(jnp.bfloat16)
        current = (NEWTON_A * wide + jnp.dot(wide, mixing.astype(jnp.float32), preferred_element_type=jnp.float32)).astype(jnp.bfloat16)
    return current

def reference(master, momentum, gradient, up_weight, down_weight, tokens, routes, route_weight):
    new_momentum = MOMENTUM_BETA * momentum + gradient.astype(jnp.float32)
    blended = (gradient.astype(jnp.float32) + MOMENTUM_BETA * new_momentum).astype(jnp.bfloat16)
    updates = lax.map(orthogonal, blended)
    step_scale = LEARN_RATE * 0.2 * math.sqrt(max(D, F))
    new_master = master * (1.0 - LEARN_RATE * WEIGHT_DECAY) - step_scale * updates.astype(jnp.float32)
    live_gate = new_master.astype(jnp.bfloat16)
    positions = jnp.arange(TOKENS, dtype=jnp.int32)

    def expert_step(totals, inputs):
        gate_matrix, up_matrix, down_matrix, expert = inputs
        matches = routes == expert
        member = jnp.any(matches, axis=1)
        weights = lax.optimization_barrier(jnp.sum(jnp.where(matches, route_weight, 0.0), axis=1))
        ordering = jnp.argsort(jnp.where(member, positions, positions + TOKENS))[:CAP].astype(jnp.int32)
        picked = tokens[ordering]
        slot_weight = weights[ordering]
        gate_value = jnp.dot(picked, gate_matrix, preferred_element_type=jnp.float32)
        upward = jnp.dot(picked, up_matrix.T, preferred_element_type=jnp.float32)
        hidden = (jax.nn.silu(gate_value) * upward).astype(jnp.bfloat16)
        output = jnp.dot(hidden, down_matrix, preferred_element_type=jnp.float32)
        totals = totals.at[ordering].add(output * slot_weight[:, None])
        return (totals, None)
    start_totals = jnp.zeros((TOKENS, D), jnp.float32)
    expert_ids = jnp.arange(EXPERTS, dtype=jnp.int32)
    totals, unused = lax.scan(expert_step, start_totals, (live_gate, up_weight, down_weight, expert_ids))
    return (new_master, new_momentum, totals.astype(jnp.bfloat16))
```

```python
import functools
import math

import jax
import jax.numpy as jnp
from jax import lax
from jax.experimental import pallas as pl
from jax.experimental.pallas import tpu as pltpu
from jax.sharding import PartitionSpec as P

NS_ITERS = 5
MOMENTUM_BETA = 0.95
LEARN_RATE = 0.08
WEIGHT_DECAY = 0.1
NEWTON_A = 3.4445
NEWTON_B = -4.775
NEWTON_C = 2.0315
EPSILON = 1e-07
BLOCK = 256


f32 = jnp.float32
bf16 = jnp.bfloat16


def dot_nn(a, b):
    return jnp.dot(a, b, preferred_element_type=f32)


def dot_nt(a, b):
    return lax.dot_general(a, b, (((1,), (1,)), ((), ())), preferred_element_type=f32)


def newton_kernel(own_count, other_count, *refs):
    own = refs[:own_count]
    other = refs[own_count : own_count + other_count]
    tokens = refs[own_count + other_count]
    rest = refs[own_count + other_count + 1 :]
    finals, token_out = rest[:own_count], rest[own_count]
    xt, gram_wide, gram, mixing = rest[own_count + 1 :]
    features = xt.shape[0]
    rows = own[0].shape[0]
    blocks = [(j, min(j + BLOCK, features)) for j in range(0, features, BLOCK)]

    for at, piece in enumerate(own + other):
        xt[:, at * rows : (at + 1) * rows] = piece[...].T

    def mirror(ref):
        for lo, hi in blocks:
            for low, high in blocks:
                if low > lo:
                    ref[lo:hi, low:high] = ref[low:high, lo:hi].T

    def fill_gram(target):
        for lo, hi in blocks:
            target[lo:, lo:hi] = dot_nt(xt[lo:, :], xt[lo:hi, :]).astype(target.dtype)

    def fill_mixing():
        mirror(gram)
        for lo, hi in blocks:
            square = dot_nn(gram[lo:, :], gram[:, lo:hi])
            mixing[lo:, lo:hi] = (
                NEWTON_B * gram[lo:, lo:hi].astype(f32) + NEWTON_C * square
            ).astype(bf16)
        mirror(mixing)

    def stepped(x):
        return NEWTON_A * x.astype(f32) + dot_nn(mixing[...], x)

    fill_gram(gram_wide)
    trace = jnp.zeros((1, 1), f32)
    for lo, hi in blocks:
        shape = (hi - lo, hi - lo)
        diagonal = lax.broadcasted_iota(jnp.int32, shape, 0) == lax.broadcasted_iota(
            jnp.int32, shape, 1
        )
        trace = trace + jnp.sum(jnp.where(diagonal, gram_wide[lo:hi, lo:hi], 0.0))
    inverse = 1.0 / (jnp.sqrt(trace) + EPSILON)
    for lo, hi in blocks:
        gram[lo:, lo:hi] = (gram_wide[lo:, lo:hi] * inverse * inverse).astype(bf16)
    fill_mixing()
    xt[...] = (stepped(xt[...]) * inverse).astype(bf16)

    def iteration(index, carry):
        fill_gram(gram)
        fill_mixing()
        xt[...] = stepped(xt[...]).astype(bf16)
        return carry

    lax.fori_loop(0, NS_ITERS - 2, iteration, 0)

    fill_gram(gram)
    fill_mixing()
    for at in range(own_count):
        final = stepped(xt[:, at * rows : (at + 1) * rows]).astype(bf16)
        finals[at][...] = final.T
    projected = dot_nt(tokens[...], xt[...])
    token_out[...] = NEWTON_A * projected + dot_nn(projected.astype(bf16), mixing[...])


def newton(own, other, tokens):
    rows, features = own[0].shape
    total = rows * (len(own) + len(other))
    results = pl.pallas_call(
        functools.partial(newton_kernel, len(own), len(other)),
        out_shape=[jax.ShapeDtypeStruct((rows, features), bf16)] * len(own)
        + [jax.ShapeDtypeStruct((tokens.shape[0], features), f32)],
        scratch_shapes=[
            pltpu.VMEM((features, total), bf16),
            pltpu.VMEM((features, features), f32),
            pltpu.VMEM((features, features), bf16),
            pltpu.VMEM((features, features), bf16),
        ],
        compiler_params=pltpu.CompilerParams(vmem_limit_bytes=40 << 20),
        cost_estimate=pl.CostEstimate(
            flops=2 * NS_ITERS * (2 * total * features**2 + features**3),
            bytes_accessed=4 * total * features,
            transcendentals=0,
        ),
        name="newton",
    )(*own, *other, tokens)
    return results[:-1], results[-1]


def body(master, momentum, gradient, up_weight, down_weight, tokens, routes, route_weight):
    shards, sides, groups = (lax.axis_size(n) for n in ("shard", "side", "group"))
    shard, side, group = (lax.axis_index(n) for n in ("shard", "side", "group"))
    experts, rows, features = master.shape
    local = experts // shards
    count, width = tokens.shape
    half = features // sides
    step_scale = LEARN_RATE * 0.2 * math.sqrt(max(width, features))
    order = list(range(shards - 1, -1, -1))

    def swap(value, axis, offset):
        size = lax.axis_size(axis)
        return lax.ppermute(value, axis, [(i, i ^ offset) for i in range(size)])

    def part(value, index, size, dim=0):
        return lax.dynamic_slice_in_dim(value, index * size, size, dim)

    pieces = {}
    for offset in order:
        at = shard ^ offset
        grad = part(gradient, at, local).astype(f32)
        moment = MOMENTUM_BETA * part(momentum, at, local) + grad
        pieces[offset] = (grad + MOMENTUM_BETA * moment).astype(bf16)
    own = {offset: swap(pieces[offset], "shard", offset) if offset else pieces[offset] for offset in order}
    other = [swap(own[offset], "side", q) for q in range(1, sides) for offset in range(shards)]
    new_momentum = MOMENTUM_BETA * momentum + gradient.astype(f32)

    def sorted_rows(value):
        tail = value.shape[1:]
        split = value.reshape((groups, shards, sides, -1) + tail)
        return jnp.moveaxis(split, 2, 0).reshape((count,) + tail)

    tokens = sorted_rows(tokens)
    routes = sorted_rows(routes)
    route_weight = sorted_rows(route_weight)
    row_tokens = part(tokens, shard * sides + side, rows, 1)
    decayed = ((1.0 - LEARN_RATE * WEIGHT_DECAY) * master).astype(bf16)
    base_parts = jnp.einsum(
        "tr,erf->etf", row_tokens, decayed, preferred_element_type=f32
    ).astype(bf16)
    base = part(base_parts, shard, local).astype(f32)
    for offset in range(1, shards):
        base = base + swap(part(base_parts, shard ^ offset, local), "shard", offset).astype(f32)
    upward = jnp.einsum("td,efd->etf", tokens, up_weight, preferred_element_type=f32)
    first = (group * shards + shard) * local
    expert_ids = first + jnp.arange(local, dtype=jnp.int32)
    matches = routes[None, :, :] == expert_ids[:, None, None]
    weights = jnp.sum(jnp.where(matches, route_weight[None, :, :], 0.0), axis=2)
    feature_order = [(shard ^ o) * sides + (side ^ q) for q in range(sides) for o in range(shards)]
    piece_tokens = jnp.concatenate([part(tokens, i, rows, 1) for i in feature_order], axis=1)

    finals, token_outs = [], []
    for e in range(local):
        final, token_out = newton(
            [own[o][e] for o in range(shards)], [piece[e] for piece in other], piece_tokens
        )
        finals.append(final)
        token_outs.append(token_out)
    returned = {}
    for offset in order:
        block = jnp.stack([final[offset] for final in finals])
        returned[offset] = swap(block, "shard", offset) if offset else block

    kept = part(base, side, half, 2)
    for q in range(1, sides):
        kept = kept + swap(part(base, side ^ q, half, 2).astype(bf16), "side", q).astype(f32)
    gate = kept - step_scale * part(jnp.stack(token_outs), side, half, 2)
    hidden = (jax.nn.silu(gate) * upward).astype(bf16)
    output = jnp.einsum("etf,efd->etd", hidden, down_weight, preferred_element_type=f32)
    partial = jnp.sum(output * weights[:, :, None], axis=0)
    for axis, index, size in (("side", side, sides), ("group", group, groups), ("shard", shard, shards)):
        block = partial.shape[0] // size
        sent = partial.astype(bf16)
        partial = part(partial, index, block)
        for offset in range(1, size):
            partial = partial + swap(part(sent, index ^ offset, block), axis, offset).astype(f32)
    combined = partial.astype(bf16)

    new_master = jnp.zeros_like(master)
    for offset in reversed(order):
        at = (shard ^ offset) * local
        old = lax.dynamic_slice_in_dim(master, at, local, 0)
        new = old * (1.0 - LEARN_RATE * WEIGHT_DECAY) - step_scale * returned[offset].astype(f32)
        new_master = lax.dynamic_update_slice_in_dim(new_master, new, at, 0)
    return (new_master, new_momentum, combined)


def solution(mesh):
    in_specs = (
        P("group", ("shard", "side"), None),
        P("group", ("shard", "side"), None),
        P("group", ("shard", "side"), None),
        P(("group", "shard"), "side", None),
        P(("group", "shard"), "side", None),
        P(),
        P(),
        P(),
    )
    out_specs = (
        P("group", ("shard", "side"), None),
        P("group", ("shard", "side"), None),
        P(("group", "shard", "side"), None),
    )
    return jax.shard_map(body, mesh=mesh, in_specs=in_specs, out_specs=out_specs, check_vma=False)
```

```python
import functools
import math

import jax
import jax.numpy as jnp
import numpy as np
from jax import lax
from jax.experimental import pallas as pl
from jax.experimental.pallas import tpu as pltpu
from jax.sharding import PartitionSpec as P

NS_ITERS = 5
MOMENTUM_BETA = 0.95
LEARN_RATE = 0.08
WEIGHT_DECAY = 0.1
NEWTON_A = 3.4445
NEWTON_B = -4.775
NEWTON_C = 2.0315
EPSILON = 1e-07
BLOCK = 256


f32 = jnp.float32
bf16 = jnp.bfloat16


def dot_nn(a, b):
    return jnp.dot(a, b, preferred_element_type=f32)


def dot_nt(a, b):
    return lax.dot_general(a, b, (((1,), (1,)), ((), ())), preferred_element_type=f32)


def newton_kernel(own_count, other_count, *refs):
    places, refs = refs[0], refs[1:]
    own = refs[:own_count]
    other = refs[own_count : own_count + other_count]
    tokens = refs[own_count + other_count]
    rest = refs[own_count + other_count + 1 :]
    finals, token_out = rest[:own_count], rest[own_count]
    xt, gram_wide, gram, mixing = rest[own_count + 1 :]
    features = xt.shape[0]
    rows = own[0].shape[0]
    blocks = [(j, min(j + BLOCK, features)) for j in range(0, features, BLOCK)]

    for at, piece in enumerate(own + other):
        xt[:, at * rows : (at + 1) * rows] = piece[...].T

    def mirror(ref):
        for lo, hi in blocks:
            for low, high in blocks:
                if low > lo:
                    ref[lo:hi, low:high] = ref[low:high, lo:hi].T

    def fill_gram(target):
        for lo, hi in blocks:
            target[lo:, lo:hi] = dot_nt(xt[lo:, :], xt[lo:hi, :]).astype(target.dtype)

    def fill_mixing():
        mirror(gram)
        for lo, hi in blocks:
            square = dot_nn(gram[lo:, :], gram[:, lo:hi])
            mixing[lo:, lo:hi] = (
                NEWTON_B * gram[lo:, lo:hi].astype(f32) + NEWTON_C * square
            ).astype(bf16)
        mirror(mixing)

    def stepped(x):
        return NEWTON_A * x.astype(f32) + dot_nn(mixing[...], x)

    fill_gram(gram_wide)
    trace = jnp.zeros((1, 1), f32)
    for lo, hi in blocks:
        shape = (hi - lo, hi - lo)
        diagonal = lax.broadcasted_iota(jnp.int32, shape, 0) == lax.broadcasted_iota(
            jnp.int32, shape, 1
        )
        trace = trace + jnp.sum(jnp.where(diagonal, gram_wide[lo:hi, lo:hi], 0.0))
    inverse = 1.0 / (jnp.sqrt(trace) + EPSILON)
    for lo, hi in blocks:
        gram[lo:, lo:hi] = (gram_wide[lo:, lo:hi] * inverse * inverse).astype(bf16)
    fill_mixing()
    xt[...] = (stepped(xt[...]) * inverse).astype(bf16)

    def iteration(index, carry):
        fill_gram(gram)
        fill_mixing()
        xt[...] = stepped(xt[...]).astype(bf16)
        return carry

    lax.fori_loop(0, NS_ITERS - 2, iteration, 0)

    fill_gram(gram)
    fill_mixing()
    for at in range(own_count):
        final = stepped(xt[:, at * rows : (at + 1) * rows]).astype(bf16)
        finals[at][...] = final.T
    projected = jnp.zeros(token_out.shape, f32)
    for at in range(own_count + other_count):
        columns = pl.ds(pl.multiple_of(places[at] * rows, rows), rows)
        projected += dot_nt(tokens[:, columns], xt[:, at * rows : (at + 1) * rows])
    token_out[...] = NEWTON_A * projected + dot_nn(projected.astype(bf16), mixing[...])


def newton(places, own, other, tokens):
    rows, features = own[0].shape
    total = rows * (len(own) + len(other))
    whole = pl.BlockSpec(memory_space=pltpu.VMEM)
    count = len(own) + len(other)
    results = pl.pallas_call(
        functools.partial(newton_kernel, len(own), len(other)),
        out_shape=[jax.ShapeDtypeStruct((rows, features), bf16)] * len(own)
        + [jax.ShapeDtypeStruct((tokens.shape[0], features), f32)],
        in_specs=[pl.BlockSpec(memory_space=pltpu.SMEM)] + [whole] * count + [whole],
        out_specs=[whole] * len(own) + [whole],
        scratch_shapes=[
            pltpu.VMEM((features, total), bf16),
            pltpu.VMEM((features, features), f32),
            pltpu.VMEM((features, features), bf16),
            pltpu.VMEM((features, features), bf16),
        ],
        compiler_params=pltpu.CompilerParams(vmem_limit_bytes=24 << 20),
        cost_estimate=pl.CostEstimate(
            flops=2 * NS_ITERS * (2 * total * features**2 + features**3),
            bytes_accessed=4 * total * features,
            transcendentals=0,
        ),
        name="newton",
    )(places, *own, *other, tokens)
    return results[:-1], results[-1]


def base_kernel(sides, place, tokens, master, keep, *sends):
    half = keep.shape[2]
    for e in range(master.shape[0]):
        decayed = ((1.0 - LEARN_RATE * WEIGHT_DECAY) * master[e]).astype(bf16)
        product = dot_nn(tokens[...], decayed).astype(bf16)
        for q in range(sides):

            @pl.when(place[1] == q)
            def _():
                keep[e] = product[:, q * half : (q + 1) * half]
                for k in range(1, sides):
                    p = q ^ k
                    sends[k - 1][e] = product[:, p * half : (p + 1) * half]


def base_products(place, tokens, master, sides):
    experts, rows, features = master.shape
    count, half = tokens.shape[0], features // sides
    batch = math.gcd(experts, 2)
    out = pl.BlockSpec((batch, count, half), lambda e, place: (e, 0, 0))
    return pl.pallas_call(
        functools.partial(base_kernel, sides),
        out_shape=[jax.ShapeDtypeStruct((experts, count, half), bf16)] * sides,
        grid_spec=pltpu.PrefetchScalarGridSpec(
            num_scalar_prefetch=1,
            grid=(experts // batch,),
            in_specs=[
                pl.BlockSpec((count, rows), lambda e, place: (0, place[0])),
                pl.BlockSpec((batch, rows, features), lambda e, place: (e, 0, 0)),
            ],
            out_specs=[out] * sides,
        ),
        compiler_params=pltpu.CompilerParams(vmem_limit_bytes=12 << 20),
        cost_estimate=pl.CostEstimate(
            flops=2 * experts * count * rows * features,
            bytes_accessed=4 * experts * rows * features,
            transcendentals=0,
        ),
        name="base",
    )(place, tokens, master)


def fold_kernel(parts, place, *refs):
    terms, outs = refs[:parts], refs[parts:]
    size, block = len(outs), outs[0].shape[0]
    aligned = terms[0].ndim > 2 or block % 8 == 0

    def write(index):
        for offset in range(size):
            at = index ^ offset
            if aligned:
                rows = pl.ds(pl.multiple_of(at * block, block), block)
            else:
                rows = slice(at * block, (at + 1) * block)
            total = terms[0][rows].astype(f32)
            for term in terms[1:]:
                total = total + term[rows].astype(f32)
            outs[offset][...] = total.astype(outs[offset].dtype)

    if aligned:
        write(place[0])
    else:
        for index in range(size):
            pl.when(place[0] == index)(functools.partial(write, index))


def fold(terms, index, size, own_type):
    shape = (terms[0].shape[0] // size,) + terms[0].shape[1:]
    whole = pl.BlockSpec(memory_space=pltpu.VMEM)
    return pl.pallas_call(
        functools.partial(fold_kernel, len(terms)),
        out_shape=[jax.ShapeDtypeStruct(shape, own_type if k == 0 else bf16) for k in range(size)],
        in_specs=[pl.BlockSpec(memory_space=pltpu.SMEM)] + [whole] * len(terms),
        out_specs=[whole] * size,
        compiler_params=pltpu.CompilerParams(vmem_limit_bytes=12 << 20),
        cost_estimate=pl.CostEstimate(
            flops=terms[0].size * len(terms), bytes_accessed=4 * terms[0].size, transcendentals=0
        ),
        name="fold",
    )(index, *terms)


def roll_kernel(pieces, step_scale, places, *refs):
    base = refs[:pieces]
    token_out, upward, down, routes, route_weight, source, keep = refs[pieces : pieces + 7]
    sends = refs[pieces + 7 :]
    local, count, half = upward.shape
    columns = pl.ds(pl.multiple_of(places[1] * half, half), half)
    index = lax.broadcasted_iota(jnp.int32, (count, count), 1)
    sorting = index == source[...]
    total = jnp.zeros((count, down.shape[2]), f32)
    for e in range(local):
        gate = -step_scale * token_out[e, :, columns]
        for piece in base:
            gate = gate + piece[e].astype(f32)
        hidden = (gate / (1.0 + jnp.exp(-gate)) * upward[e]).astype(bf16)
        hidden = dot_nn(sorting.astype(bf16), hidden).astype(bf16)
        chosen = routes[...] == places[0] + e
        weight = jnp.sum(jnp.where(chosen, route_weight[...], 0.0), axis=0, keepdims=True)
        weight = jnp.sum(jnp.where(sorting, weight, 0.0), axis=1, keepdims=True)
        total = total + dot_nn(hidden, down[e]) * weight
    block = keep.shape[0]
    side = places[1]
    for q in range(count // block):

        @pl.when(side == q)
        def _():
            keep[...] = total[q * block : (q + 1) * block]
            for k in range(1, count // block):
                p = q ^ k
                sends[k - 1][...] = total[p * block : (p + 1) * block].astype(bf16)


def rollout(places, base, token_out, upward, down, routes, route_weight, source, sides, step_scale):
    local, count, half = upward.shape
    width = down.shape[2]
    whole = pl.BlockSpec(memory_space=pltpu.VMEM)
    return pl.pallas_call(
        functools.partial(roll_kernel, len(base), step_scale),
        out_shape=[
            jax.ShapeDtypeStruct((count // sides, width), f32 if q == 0 else bf16)
            for q in range(sides)
        ],
        in_specs=[pl.BlockSpec(memory_space=pltpu.SMEM)] + [whole] * (len(base) + 6),
        out_specs=[whole] * sides,
        compiler_params=pltpu.CompilerParams(vmem_limit_bytes=20 << 20),
        cost_estimate=pl.CostEstimate(
            flops=2 * local * count * half * width,
            bytes_accessed=2 * local * half * width,
            transcendentals=0,
        ),
        name="roll",
    )(places, *base, token_out, upward, down, routes, route_weight, source)


def step(master, momentum, gradient, up_weight, down_weight, tokens, routes, route_weight):
    shards, sides, groups = (lax.axis_size(n) for n in ("shard", "side", "group"))
    shard, side, group = (lax.axis_index(n) for n in ("shard", "side", "group"))
    experts, _, features = master.shape
    local = experts // shards
    count, width = tokens.shape
    step_scale = LEARN_RATE * 0.2 * math.sqrt(max(width, features))
    away = list(range(1, shards))

    def swap(value, axis, offset):
        size = lax.axis_size(axis)
        return lax.ppermute(value, axis, [(i, i ^ offset) for i in range(size)])

    def part(value, index, size, dim=0):
        return lax.dynamic_slice_in_dim(value, index * size, size, dim)

    def scalars(*values):
        return jnp.stack([jnp.asarray(v, jnp.int32) for v in values])

    def piece(offset, moment, grad):
        at = shard ^ offset
        grad = part(grad, at, local).astype(f32)
        moment = MOMENTUM_BETA * part(moment, at, local) + grad
        return (grad + MOMENTUM_BETA * moment).astype(bf16)

    cut = (shards + 1) // 2 + 1
    near = [piece(offset, momentum, gradient) for offset in range(1, cut)]
    near, moment_in, grad_in = lax.optimization_barrier((near, momentum, gradient))
    far = [piece(offset % shards, moment_in, grad_in) for offset in range(cut, shards + 1)]
    pieces = far[-1:] + near + far[:-1]
    own = []
    for offset in range(shards):
        own.append(swap(pieces[offset], "shard", offset) if offset else pieces[offset])
    other = []
    for q in range(1, sides):
        for offset in range(shards):
            other.append(swap(own[offset], "side", q))
    new_momentum = MOMENTUM_BETA * momentum + gradient.astype(f32)

    products = base_products(
        scalars(shard * sides + side, side), tokens, master, sides
    )
    terms = [products[0]] + [swap(products[q], "side", q) for q in range(1, sides)]
    sums = fold(terms, scalars(shard), shards, bf16)
    base = [sums[0]]
    for offset in away:
        base.append(swap(sums[offset], "shard", offset))
    upward = jnp.einsum("td,efd->etf", tokens, up_weight, preferred_element_type=f32)

    own_list = own
    own_list, other, upward = lax.optimization_barrier((own_list, other, upward))
    feature_places = scalars(
        *[(shard ^ o) * sides + (side ^ q) for q in range(sides) for o in range(shards)]
    )
    finals, token_outs = [], []
    for e in range(local):
        final, token_out = newton(
            feature_places, [piece[e] for piece in own_list], [piece[e] for piece in other], tokens
        )
        finals.append(final)
        token_outs.append(token_out)
    token_outs, base = lax.optimization_barrier((token_outs, base))
    returned = []
    for offset in range(shards):
        block = jnp.stack([final[offset] for final in finals])
        returned.append(swap(block, "shard", offset) if offset else block)

    source = np.arange(count, dtype=np.int32).reshape(groups, shards, sides, -1)
    source = jnp.asarray(np.transpose(source, (2, 0, 1, 3)).reshape(count, 1))
    first = (group * shards + shard) * local
    terms = rollout(
        scalars(first, side), base, jnp.stack(token_outs), upward, down_weight,
        routes.T, route_weight.T, source, sides, step_scale,
    )
    axis = "side"
    for later, index, size in (("group", group, groups), ("shard", shard, shards)):
        terms = [terms[0]] + [swap(terms[k], axis, k) for k in range(1, len(terms))]
        terms = fold(terms, scalars(index), size, f32)
        axis = later
    combined = terms[0]
    for offset in away:
        combined = combined + swap(terms[offset], "shard", offset).astype(f32)
    combined = combined.astype(bf16)

    new_master = jnp.zeros_like(master)
    for offset in range(shards):
        at = (shard ^ offset) * local
        old = lax.dynamic_slice_in_dim(master, at, local, 0)
        new = old * (1.0 - LEARN_RATE * WEIGHT_DECAY) - step_scale * returned[offset].astype(f32)
        new_master = lax.dynamic_update_slice_in_dim(new_master, new, at, 0)
    return (new_master, new_momentum, combined)


def solution(mesh):
    in_specs = (
        P("group", ("shard", "side"), None),
        P("group", ("shard", "side"), None),
        P("group", ("shard", "side"), None),
        P(("group", "shard"), "side", None),
        P(("group", "shard"), "side", None),
        P(),
        P(),
        P(),
    )
    out_specs = (
        P("group", ("shard", "side"), None),
        P("group", ("shard", "side"), None),
        P(("group", "shard", "side"), None),
    )
    return jax.shard_map(step, mesh=mesh, in_specs=in_specs, out_specs=out_specs, check_vma=False)
```

```python
import functools
import math

import jax
import jax.numpy as jnp
import numpy as np
from jax import lax
from jax.experimental import pallas as pl
from jax.experimental.pallas import tpu as pltpu
from jax.sharding import PartitionSpec as P

NS_ITERS = 5
MOMENTUM_BETA = 0.95
LEARN_RATE = 0.08
WEIGHT_DECAY = 0.1
NEWTON_A = 3.4445
NEWTON_B = -4.775
NEWTON_C = 2.0315
EPSILON = 1e-07
BLOCK = 256


f32 = jnp.float32
bf16 = jnp.bfloat16


def dot_nn(a, b):
    return jnp.dot(a, b, preferred_element_type=f32)


def dot_nt(a, b):
    return lax.dot_general(a, b, (((1,), (1,)), ((), ())), preferred_element_type=f32)


def newton_kernel(count, early, places, tokens, *refs):
    pieces, rest = refs[:count], refs[count:]
    finals, rest = rest[: len(early)], rest[len(early) :]
    xt, mixing, token_out, gram_wide, gram = rest
    rows, features = pieces[0].shape
    blocks = [(j, min(j + BLOCK, features)) for j in range(0, features, BLOCK)]

    for at, piece in enumerate(pieces):
        xt[:features, at * rows : (at + 1) * rows] = piece[...].T
        columns = pl.ds(pl.multiple_of(places[at] * rows, rows), rows)
        xt[features:, at * rows : (at + 1) * rows] = tokens[:, columns]

    def mirror(ref):
        for lo, hi in blocks:
            for low, high in blocks:
                if low > lo:
                    ref[lo:hi, low:high] = ref[low:high, lo:hi].T

    def fill_gram(target):
        for lo, hi in blocks:
            target[lo:, lo:hi] = dot_nt(xt[lo:features, :], xt[lo:hi, :]).astype(target.dtype)

    def fill_mixing():
        mirror(gram)
        for lo, hi in blocks:
            square = dot_nn(gram[lo:, :], gram[:, lo:hi])
            mixing[lo:, lo:hi] = (
                NEWTON_B * gram[lo:, lo:hi].astype(f32) + NEWTON_C * square
            ).astype(bf16)
        mirror(mixing)

    fill_gram(gram_wide)
    trace = jnp.zeros((1, 1), f32)
    for lo, hi in blocks:
        shape = (hi - lo, hi - lo)
        diagonal = lax.broadcasted_iota(jnp.int32, shape, 0) == lax.broadcasted_iota(
            jnp.int32, shape, 1
        )
        trace = trace + jnp.sum(jnp.where(diagonal, gram_wide[lo:hi, lo:hi], 0.0))
    inverse = 1.0 / (jnp.sqrt(trace) + EPSILON)
    for lo, hi in blocks:
        gram[lo:, lo:hi] = (gram_wide[lo:, lo:hi] * inverse * inverse).astype(bf16)
    fill_mixing()
    xt[:features] = (stepped(mixing, xt[:features]) * inverse).astype(bf16)

    def iteration(index, carry):
        fill_gram(gram)
        fill_mixing()
        xt[:features] = stepped(mixing, xt[:features]).astype(bf16)
        return carry

    lax.fori_loop(0, NS_ITERS - 2, iteration, 0)

    for lo, hi in blocks:
        product = dot_nt(xt[lo:, :], xt[lo:hi, :])
        gram[lo:, lo:hi] = product[: features - lo].astype(bf16)
        token_out[:, lo:hi] = product[features - lo :]
    fill_mixing()
    apply_last(xt, mixing, rows, early, finals)


def stepped(mixing, x):
    return NEWTON_A * x.astype(f32) + dot_nn(mixing[...], x)


def apply_last(xt, mixing, rows, chosen, finals):
    for at, final in zip(chosen, finals):
        final[...] = stepped(
            mixing, xt[: mixing.shape[0], at * rows : (at + 1) * rows]
        ).astype(bf16).T


def finish_kernel(rows, late, xt, mixing, *finals):
    apply_last(xt, mixing, rows, late, finals)


def newton(places, tokens, pieces, early):
    rows, features = pieces[0].shape
    total = rows * len(pieces)
    whole = pl.BlockSpec(memory_space=pltpu.VMEM)
    results = pl.pallas_call(
        functools.partial(newton_kernel, len(pieces), early),
        out_shape=[jax.ShapeDtypeStruct((rows, features), bf16)] * len(early)
        + [
            jax.ShapeDtypeStruct((features + tokens.shape[0], total), bf16),
            jax.ShapeDtypeStruct((features, features), bf16),
            jax.ShapeDtypeStruct((tokens.shape[0], features), f32),
        ],
        in_specs=[pl.BlockSpec(memory_space=pltpu.SMEM)] + [whole] * (len(pieces) + 1),
        out_specs=[whole] * (len(early) + 3),
        scratch_shapes=[
            pltpu.VMEM((features, features), f32),
            pltpu.VMEM((features, features), bf16),
        ],
        compiler_params=pltpu.CompilerParams(vmem_limit_bytes=24 << 20),
        cost_estimate=pl.CostEstimate(
            flops=2 * NS_ITERS * (2 * total * features**2 + features**3),
            bytes_accessed=4 * total * features,
            transcendentals=0,
        ),
        name="newton",
    )(places, tokens, *pieces)
    return results[:-3], *results[-3:]


def finish(xt, mixing, rows, late):
    features = mixing.shape[0]
    whole = pl.BlockSpec(memory_space=pltpu.VMEM)
    return pl.pallas_call(
        functools.partial(finish_kernel, rows, late),
        out_shape=[jax.ShapeDtypeStruct((rows, features), bf16)] * len(late),
        in_specs=[whole] * 2,
        out_specs=[whole] * len(late),
        compiler_params=pltpu.CompilerParams(vmem_limit_bytes=16 << 20),
        cost_estimate=pl.CostEstimate(
            flops=2 * len(late) * rows * features**2,
            bytes_accessed=4 * xt.size,
            transcendentals=0,
        ),
        name="finish",
    )(xt, mixing)


def base_kernel(sides, place, tokens, master, keep, *sends):
    half = keep.shape[2]
    for e in range(master.shape[0]):
        decayed = ((1.0 - LEARN_RATE * WEIGHT_DECAY) * master[e]).astype(bf16)
        product = dot_nn(tokens[...], decayed).astype(bf16)
        for q in range(sides):

            @pl.when(place[1] == q)
            def _():
                keep[e] = product[:, q * half : (q + 1) * half]
                for k in range(1, sides):
                    p = q ^ k
                    sends[k - 1][e] = product[:, p * half : (p + 1) * half]


def base_products(place, tokens, master, sides):
    experts, rows, features = master.shape
    count, half = tokens.shape[0], features // sides
    batch = math.gcd(experts, 2)
    out = pl.BlockSpec((batch, count, half), lambda e, place: (e, 0, 0))
    return pl.pallas_call(
        functools.partial(base_kernel, sides),
        out_shape=[jax.ShapeDtypeStruct((experts, count, half), bf16)] * sides,
        grid_spec=pltpu.PrefetchScalarGridSpec(
            num_scalar_prefetch=1,
            grid=(experts // batch,),
            in_specs=[
                pl.BlockSpec((count, rows), lambda e, place: (0, place[0])),
                pl.BlockSpec((batch, rows, features), lambda e, place: (e, 0, 0)),
            ],
            out_specs=[out] * sides,
        ),
        compiler_params=pltpu.CompilerParams(vmem_limit_bytes=12 << 20),
        cost_estimate=pl.CostEstimate(
            flops=2 * experts * count * rows * features,
            bytes_accessed=4 * experts * rows * features,
            transcendentals=0,
        ),
        name="base",
    )(place, tokens, master)


def fold_kernel(parts, place, *refs):
    terms, outs = refs[:parts], refs[parts:]
    size, block = len(outs), outs[0].shape[0]
    aligned = terms[0].ndim > 2 or block % 8 == 0

    def write(index):
        for offset in range(size):
            at = index ^ offset
            if aligned:
                rows = pl.ds(pl.multiple_of(at * block, block), block)
            else:
                rows = slice(at * block, (at + 1) * block)
            total = terms[0][rows].astype(f32)
            for term in terms[1:]:
                total = total + term[rows].astype(f32)
            outs[offset][...] = total.astype(outs[offset].dtype)

    if aligned:
        write(place[0])
    else:
        for index in range(size):
            pl.when(place[0] == index)(functools.partial(write, index))


def fold(terms, index, size, own_type):
    shape = (terms[0].shape[0] // size,) + terms[0].shape[1:]
    whole = pl.BlockSpec(memory_space=pltpu.VMEM)
    return pl.pallas_call(
        functools.partial(fold_kernel, len(terms)),
        out_shape=[jax.ShapeDtypeStruct(shape, own_type if k == 0 else bf16) for k in range(size)],
        in_specs=[pl.BlockSpec(memory_space=pltpu.SMEM)] + [whole] * len(terms),
        out_specs=[whole] * size,
        compiler_params=pltpu.CompilerParams(vmem_limit_bytes=12 << 20),
        cost_estimate=pl.CostEstimate(
            flops=terms[0].size * len(terms), bytes_accessed=4 * terms[0].size, transcendentals=0
        ),
        name="fold",
    )(index, *terms)


def roll_kernel(pieces, step_scale, places, *refs):
    base = refs[:pieces]
    token_out, mixing, upward, down, routes, route_weight, source, keep = refs[pieces : pieces + 8]
    sends = refs[pieces + 8 :]
    local, count, half = upward.shape
    columns = pl.ds(pl.multiple_of(places[1] * half, half), half)
    index = lax.broadcasted_iota(jnp.int32, (count, count), 1)
    sorting = index == source[...]
    total = jnp.zeros((count, down.shape[2]), f32)
    for e in range(local):
        gate = NEWTON_A * token_out[e, :, columns]
        gate += dot_nn(token_out[e].astype(bf16), mixing[e, :, columns])
        gate = -step_scale * gate
        for piece in base:
            gate = gate + piece[e].astype(f32)
        hidden = (gate / (1.0 + jnp.exp(-gate)) * upward[e]).astype(bf16)
        hidden = dot_nn(sorting.astype(bf16), hidden).astype(bf16)
        chosen = routes[...] == places[0] + e
        weight = jnp.sum(jnp.where(chosen, route_weight[...], 0.0), axis=0, keepdims=True)
        weight = jnp.sum(jnp.where(sorting, weight, 0.0), axis=1, keepdims=True)
        total = total + dot_nn(hidden, down[e]) * weight
    block = keep.shape[0]
    side = places[1]
    for q in range(count // block):

        @pl.when(side == q)
        def _():
            keep[...] = total[q * block : (q + 1) * block]
            for k in range(1, count // block):
                p = q ^ k
                sends[k - 1][...] = total[p * block : (p + 1) * block].astype(bf16)


def rollout(places, base, token_out, mixing, upward, down, routes, route_weight, source, sides, step_scale):
    local, count, half = upward.shape
    width = down.shape[2]
    whole = pl.BlockSpec(memory_space=pltpu.VMEM)
    return pl.pallas_call(
        functools.partial(roll_kernel, len(base), step_scale),
        out_shape=[
            jax.ShapeDtypeStruct((count // sides, width), f32 if q == 0 else bf16)
            for q in range(sides)
        ],
        in_specs=[pl.BlockSpec(memory_space=pltpu.SMEM)] + [whole] * (len(base) + 7),
        out_specs=[whole] * sides,
        compiler_params=pltpu.CompilerParams(vmem_limit_bytes=20 << 20),
        cost_estimate=pl.CostEstimate(
            flops=2 * local * count * half * width,
            bytes_accessed=2 * local * half * width,
            transcendentals=0,
        ),
        name="roll",
    )(places, *base, token_out, mixing, upward, down, routes, route_weight, source)


def step(master, momentum, gradient, up_weight, down_weight, tokens, routes, route_weight):
    shards, sides, groups = (lax.axis_size(n) for n in ("shard", "side", "group"))
    shard, side, group = (lax.axis_index(n) for n in ("shard", "side", "group"))
    experts, rows, features = master.shape
    local = experts // shards
    count, width = tokens.shape
    step_scale = LEARN_RATE * 0.2 * math.sqrt(max(width, features))
    away = list(range(1, shards))

    def swap(value, axis, offset):
        size = lax.axis_size(axis)
        return lax.ppermute(value, axis, [(i, i ^ offset) for i in range(size)])

    def part(value, index, size, dim=0):
        return lax.dynamic_slice_in_dim(value, index * size, size, dim)

    def scalars(*values):
        return jnp.stack([jnp.asarray(v, jnp.int32) for v in values])

    def piece(offset, moment, grad):
        at = shard ^ offset
        grad = part(grad, at, local).astype(f32)
        moment = MOMENTUM_BETA * part(moment, at, local) + grad
        return (grad + MOMENTUM_BETA * moment).astype(bf16)

    cut = (shards + 1) // 2 + 1
    near = [piece(offset, momentum, gradient) for offset in range(1, cut)]
    near, moment_in, grad_in = lax.optimization_barrier((near, momentum, gradient))
    far = [piece(offset % shards, moment_in, grad_in) for offset in range(cut, shards + 1)]
    pieces = far[-1:] + near + far[:-1]
    own = []
    for offset in range(shards):
        own.append(swap(pieces[offset], "shard", offset) if offset else pieces[offset])
    other = []
    for q in range(1, sides):
        for offset in range(shards):
            other.append(swap(own[offset], "side", q))
    new_momentum = MOMENTUM_BETA * momentum + gradient.astype(f32)

    products = base_products(
        scalars(shard * sides + side, side), tokens, master, sides
    )
    terms = [products[0]] + [swap(products[q], "side", q) for q in range(1, sides)]
    sums = fold(terms, scalars(shard), shards, bf16)
    base = [sums[0]]
    for offset in away:
        base.append(swap(sums[offset], "shard", offset))
    upward = jnp.einsum("td,efd->etf", tokens, up_weight, preferred_element_type=f32)

    own_list = own
    own_list, other, upward = lax.optimization_barrier((own_list, other, upward))
    feature_places = scalars(
        *[(shard ^ o) * sides + (side ^ q) for q in range(sides) for o in range(shards)]
    )
    early = away[:-1]
    late = [offset for offset in range(shards) if offset not in early]
    cores = [
        newton(feature_places, tokens, [piece[e] for piece in own_list + other], early)
        for e in range(local)
    ]
    mixings = [core[2] for core in cores]
    token_outs = [core[3] for core in cores]
    ends = []
    for e in range(local):
        ends.append((finish(*cores[e][1:3], rows, late),))
    token_outs, base = lax.optimization_barrier((token_outs, base))
    returned = []
    for offset in range(shards):
        kind, chosen = (cores, early) if offset in early else (ends, late)
        block = jnp.stack([part_of[0][chosen.index(offset)] for part_of in kind])
        returned.append(swap(block, "shard", offset) if offset else block)

    source = np.arange(count, dtype=np.int32).reshape(groups, shards, sides, -1)
    source = jnp.asarray(np.transpose(source, (2, 0, 1, 3)).reshape(count, 1))
    first = (group * shards + shard) * local
    terms = rollout(
        scalars(first, side), base, jnp.stack(token_outs), jnp.stack(mixings), upward, down_weight,
        routes.T, route_weight.T, source, sides, step_scale,
    )
    axis = "side"
    for later, index, size in (("group", group, groups), ("shard", shard, shards)):
        received = []
        for k in range(1, len(terms)):
            received.append(swap(terms[k], axis, k))
        terms = fold([terms[0], *received], scalars(index), size, f32)
        axis = later
    combined = terms[0]
    for offset in away:
        combined = combined + swap(terms[offset], "shard", offset).astype(f32)
    combined = combined.astype(bf16)

    new_master = jnp.zeros_like(master)
    for offset in range(shards):
        at = (shard ^ offset) * local
        old = lax.dynamic_slice_in_dim(master, at, local, 0)
        new = old * (1.0 - LEARN_RATE * WEIGHT_DECAY) - step_scale * returned[offset].astype(f32)
        new_master = lax.dynamic_update_slice_in_dim(new_master, new, at, 0)
    return (new_master, new_momentum, combined)


def solution(mesh):
    in_specs = (
        P("group", ("shard", "side"), None),
        P("group", ("shard", "side"), None),
        P("group", ("shard", "side"), None),
        P(("group", "shard"), "side", None),
        P(("group", "shard"), "side", None),
        P(),
        P(),
        P(),
    )
    out_specs = (
        P("group", ("shard", "side"), None),
        P("group", ("shard", "side"), None),
        P(("group", "shard", "side"), None),
    )
    return jax.shard_map(step, mesh=mesh, in_specs=in_specs, out_specs=out_specs, check_vma=False)
```
